32 devices in a mesh: rep: 1, dp: 32 (over x, y, z, core).
Axes of the slice: x: 2, y: 2, z: 4, core: 2. Of those that a mesh axis runs over, the one named last changes fastest.
Arguments:
- x: bfloat16 [32, 2048, 1024], P(('rep', 'dp'))
- dy: bfloat16 [32, 2048, 1024], P(('rep', 'dp'))
- w_gate: bfloat16 [2, 1024, 3200], P(None, 'dp')
- w_up: bfloat16 [2, 1024, 3200], P(None, 'dp')
- w_down: bfloat16 [2, 3200, 1024], P(None, 'dp')
Outputs:
- output 1: bfloat16 [32, 2048, 1024], P(('rep', 'dp'))
- output 2: bfloat16 [2, 1024, 3200], P('rep', 'dp')
- output 3: bfloat16 [2, 1024, 3200], P('rep', 'dp')
- output 4: bfloat16 [2, 3200, 1024], P('rep', 'dp')
All inputs are finite; a program needn't handle non-finite values.
Results may differ from the reference program's by a relative error of at most 0.018.
Values are sent between devices in bfloat16 or wider.
A program may use at most 2 GiB of HBM per device.

```python
import jax
import jax.numpy as jnp
from jax import lax

SEQUENCES = 32
TOKENS = 2048
D = 1024
FF = 3200
LAYERS = 2
NAMES = ("w_gate", "w_up", "w_down")
SHAPES = {"w_gate": (LAYERS, D, FF), "w_up": (LAYERS, D, FF), "w_down": (LAYERS, FF, D)}


def bump(key, n, height):
    away = (jnp.arange(n, dtype=jnp.int32) - jax.random.randint(key, (), 0, n, jnp.int32)) % n
    return jnp.where(away < n // 8, height, 1.0)


def together(key, own, strength):
    shared = jax.random.normal(key, own.shape[1:], jnp.float32)
    return (own + strength * shared) * lax.rsqrt(1 + strength * strength)


def setup_inputs(seed: int = 0, part: int = 0) -> dict:
    kx, kdy, ka, kb, kz, kf, kh, kl, *kw = jax.random.split(jax.random.key(seed), 8 + len(NAMES))
    kx, kdy, ka, kb = (jax.random.fold_in(k, part) for k in (kx, kdy, ka, kb))
    shape = (SEQUENCES, TOKENS, D)
    much_x, much_dy = jax.random.uniform(kz, (2,), jnp.float32, 0.0, 1.0)
    layers = 2.0 ** jax.random.uniform(kl, (LAYERS, 1, 1), jnp.float32, -1.0, 1.0)
    x = together(ka, jax.random.normal(kx, shape, jnp.float32), much_x) * bump(kf, D, 4.0)
    dy = together(kb, jax.random.normal(kdy, shape, jnp.float32), much_dy)
    drawn = {"x": x.astype(jnp.bfloat16), "dy": (dy * (SEQUENCES * TOKENS) ** -0.5).astype(jnp.bfloat16)}
    for key, name in zip(kw, NAMES, strict=True):
        w = jax.random.normal(key, SHAPES[name], jnp.float32) * SHAPES[name][1] ** -0.5
        drawn[name] = (w * {"w_gate": 1.0, "w_up": bump(kh, FF, 4.0), "w_down": layers}[name]).astype(jnp.bfloat16)
    return drawn


def matmul(a, w):
    return jnp.dot(a, w, preferred_element_type=jnp.float32).astype(jnp.bfloat16)


def normed(h):
    wide = h.astype(jnp.float32)
    scale = lax.rsqrt(jnp.mean(wide**2, -1, keepdims=True) + 1e-6)
    return (wide * scale).astype(jnp.bfloat16)


def layer(h, w):
    a = normed(h)
    gate = jnp.dot(a, w["w_gate"], preferred_element_type=jnp.float32)
    up = jnp.dot(a, w["w_up"], preferred_element_type=jnp.float32)
    return h + matmul((jax.nn.silu(gate) * up).astype(jnp.bfloat16), w["w_down"])


def stack(weights, h):
    return lax.scan(lambda h, w: (layer(h, w), None), h, weights)[0]


def reference(x, dy, w_gate, w_up, w_down):
    weights = dict(zip(NAMES, (w_gate, w_up, w_down), strict=True))

    def take(so_far, sequence):
        h, by_y = sequence
        _, back = jax.vjp(stack, weights, h)
        by_weights, by_h = back(by_y)
        return jax.tree.map(lambda total, term: total + term.astype(jnp.float32), so_far, by_weights), by_h

    none_yet = {name: jnp.zeros(w.shape, jnp.float32) for name, w in weights.items()}
    by_weights, by_x = lax.scan(take, none_yet, (x, dy))
    return (by_x, *(by_weights[name].astype(jnp.bfloat16) for name in NAMES))
```

```python
import functools
import itertools

import jax
import jax.numpy as jnp
from jax import lax
from jax.experimental import pallas as pl
from jax.experimental.pallas import tpu as pltpu
from jax.sharding import Mesh, PartitionSpec as P

MESH = pl.DeviceIdType.MESH
F32, BF16 = jnp.float32, jnp.bfloat16
VMEM_BYTES = 66_000_000
CHIPS = 16
ROWS = 32
PAIR = 200
HALF = 512


class Place:
    def __init__(self):
        me = lax.axis_index("dp")
        self.c = lax.rem(me, 2)
        self.z = lax.rem(me // 2, 4)
        self.y = lax.rem(me // 8, 2)
        self.x = me // 16
        self.ox, self.oy, self.oc = 1 - self.x, 1 - self.y, 1 - self.c

    def chip(self, x, y, z):
        return (x * 2 + y) * 4 + z

    def away(self, i):
        return lax.rem(self.z + 4 - i, 4)

    def ahead(self, i):
        return lax.rem(self.z + i, 4)

    def device(self, x, y, z, c):
        return {"dp": self.chip(x, y, z) * 2 + c}

    def peers(self):
        out = [self.device(self.x, self.y, self.ahead(i), self.c) for i in (1, 2, 3)]
        out.append(self.device(self.ox, self.y, self.z, self.c))
        out.append(self.device(self.x, self.oy, self.z, self.c))
        out.append(self.device(self.x, self.y, self.z, self.oc))
        return out


def greet(at):
    barrier = pltpu.get_barrier_semaphore()
    peers = at.peers()
    for peer in peers:
        pl.semaphore_signal(barrier, inc=1, device_id=peer, device_id_type=MESH)
    pl.semaphore_wait(barrier, len(peers))


def remote(src, dst, send, recv, device):
    return pltpu.make_async_remote_copy(
        src_ref=src, dst_ref=dst, send_sem=send, recv_sem=recv, device_id=device, device_id_type=MESH
    )


class Gather:
    def __init__(self, at, own, whole, down, recv, other, sent):
        self.at, self.own, self.whole, self.down = at, own, whole, down
        self.recv, self.other, self.sent = recv, other, sent

    def block(self, chip, c):
        if self.down:
            return self.whole.at[pl.ds(pl.multiple_of(chip * PAIR, 8), PAIR), pl.ds(pl.multiple_of(c * HALF, HALF), HALF)]
        return self.whole.at[pl.ds(pl.multiple_of(chip * 2 * ROWS + c * ROWS, ROWS), ROWS), :]

    def push(self, src, chip, device):
        remote(src, self.block(chip, self.at.c), self.sent.at[0], self.recv.at[chip], device).start()

    def pair(self, src, chip):
        at = self.at
        remote(src, self.block(chip, at.c), self.sent.at[1], self.other, at.device(at.x, at.y, at.z, at.oc)).start()

    def landed(self, chip):
        block = self.block(chip, self.at.c)
        pltpu.make_async_copy(block, block, self.recv.at[chip]).wait()
        return block

    def lines(self):
        at = self.at
        chip = at.chip(at.x, at.y, at.z)
        for i in (1, 2, 3):
            self.push(self.own, chip, at.device(at.x, at.y, at.ahead(i), at.c))

    def stay(self):
        at = self.at
        return pltpu.make_async_copy(self.own, self.block(at.chip(at.x, at.y, at.z), at.c), self.sent.at[2])

    def mine(self):
        at = self.at
        chip = at.chip(at.x, at.y, at.z)
        self.push(self.own, chip, at.device(at.ox, at.y, at.z, at.c))
        self.push(self.own, chip, at.device(at.x, at.oy, at.z, at.c))
        self.pair(self.own, chip)
        self.stay().start()

    def column(self, i):
        at = self.at
        chip = at.chip(at.x, at.y, at.away(i))
        block = self.landed(chip)
        self.push(block, chip, at.device(at.ox, at.y, at.z, at.c))
        self.push(block, chip, at.device(at.x, at.oy, at.z, at.c))
        self.pair(block, chip)

    def plane(self, i):
        at = self.at
        chip = at.chip(at.ox, at.y, at.away(i))
        block = self.landed(chip)
        if i % 2 == 0:
            self.push(block, chip, at.device(at.x, at.oy, at.z, at.c))
        self.pair(block, chip)
        chip = at.chip(at.x, at.oy, at.away(i))
        block = self.landed(chip)
        if i % 2 == 1:
            self.push(block, chip, at.device(at.ox, at.y, at.z, at.c))
        self.pair(block, chip)

    def corner(self, i):
        at = self.at
        chip = at.chip(at.ox, at.oy, at.away(i))
        self.pair(self.landed(chip), chip)

    def half(self):
        return self.whole.at[:, pl.ds(0, HALF)] if self.down else self.whole.at[pl.ds(0, CHIPS * ROWS), :]

    def arrived(self):
        half = self.half()
        pltpu.make_async_copy(half, half, self.other).wait()
        self.stay().wait()

    def settled(self):
        half = self.half()
        pltpu.make_async_copy(half, half, self.sent.at[1]).wait()
        links = self.whole.at[pl.ds(0, 15 * PAIR), pl.ds(0, HALF)] if self.down else self.whole.at[pl.ds(0, 15 * ROWS), :]
        pltpu.make_async_copy(links, links, self.sent.at[0]).wait()


class Scatter:
    def __init__(self, at, term, down, bufs, recv, sent, out):
        self.at, self.term, self.down = at, term, down
        self.own, self.pair, self.qx, self.qy, self.fx, self.fy, self.fz = bufs
        self.recv, self.sent, self.out = recv, sent, out

    def start(self):
        at = self.at
        other = at.device(at.x, at.y, at.z, at.oc)
        if not self.down:
            remote(self.term.at[:, at.oc], self.pair, self.sent.at[0], self.recv.at[0], other).start()
            pltpu.make_async_copy(self.term.at[:, at.c], self.own, self.sent.at[1]).start()
            return
        ours, theirs = (pl.ds(pl.multiple_of(c * HALF, HALF), HALF) for c in (at.c, at.oc))
        for chip in range(CHIPS):
            rows = pl.ds(chip * PAIR, PAIR)
            remote(
                self.term.at[rows, theirs], self.pair.at[chip], self.sent.at[0], self.recv.at[0], other
            ).start()
            pltpu.make_async_copy(self.term.at[rows, ours], self.own.at[chip], self.sent.at[1]).start()

    def wait(self, buf, sem):
        pltpu.make_async_copy(buf, buf, sem).wait()

    def total(self, dst, chip, *more):
        rows, step = self.own.shape[1], 8 if self.down else 16

        @pl.loop(0, rows // step)
        def _(r):
            part = pl.ds(pl.multiple_of(r * step, step), step)
            value = self.own[chip, part].astype(F32) + self.pair[chip, part].astype(F32)
            for ref, i in more:
                value = value + ref[i, part].astype(F32)
            dst[part] = value.astype(BF16)

    def send(self, slot, chip, more, dst, k, device):
        src = self.own.at[chip]
        self.total(src, chip, *more)
        remote(src, dst, self.sent.at[2 + slot], self.recv.at[k], device).start()

    def corners(self):
        at = self.at
        self.wait(self.own, self.sent.at[1])
        self.wait(self.pair, self.recv.at[0])
        x, y = at.device(at.ox, at.y, at.z, at.c), at.device(at.x, at.oy, at.z, at.c)
        for i, j in ((2, 0), (0, 2)):
            self.send(i, at.chip(at.ox, at.oy, at.away(i)), (), self.qx.at[i // 2], 1 + i, x)
            self.send(j + 1, at.chip(at.ox, at.oy, at.away(j + 1)), (), self.qy.at[j // 2], 2 + j, y)
        for i in (0, 2):
            self.send(4 + i, at.chip(at.ox, at.y, at.away(i)), (), self.fx.at[i], 5 + i, x)
            self.send(9 + i, at.chip(at.x, at.oy, at.away(i + 1)), (), self.fy.at[i + 1], 10 + i, y)

    def sides(self):
        at = self.at
        x, y = at.device(at.ox, at.y, at.z, at.c), at.device(at.x, at.oy, at.z, at.c)
        for i, j in ((2, 0), (0, 2)):
            self.wait(self.qy.at[j // 2], self.recv.at[2 + j])
            self.send(5 + j, at.chip(at.ox, at.y, at.away(j + 1)), ((self.qy, j // 2),), self.fx.at[j + 1], 6 + j, x)
            self.wait(self.qx.at[i // 2], self.recv.at[1 + i])
            self.send(8 + i, at.chip(at.x, at.oy, at.away(i)), ((self.qx, i // 2),), self.fy.at[i], 9 + i, y)

    def column(self):
        at = self.at
        for i in (1, 2, 3):
            self.wait(self.fx.at[i], self.recv.at[5 + i])
            self.wait(self.fy.at[i], self.recv.at[9 + i])
            more = ((self.fx, i), (self.fy, i))
            to = at.device(at.x, at.y, at.away(i), at.c)
            self.send(11 + i, at.chip(at.x, at.y, at.away(i)), more, self.fz.at[i - 1], 12 + i, to)

    def finish(self):
        at = self.at
        self.wait(self.fx.at[0], self.recv.at[5])
        self.wait(self.fy.at[0], self.recv.at[9])
        for i in (1, 2, 3):
            self.wait(self.fz.at[i - 1], self.recv.at[12 + i])
        more = ((self.fx, 0), (self.fy, 0), (self.fz, 0), (self.fz, 1), (self.fz, 2))
        self.total(self.out, at.chip(at.x, at.y, at.z), *more)
        self.wait(self.pair, self.sent.at[0])
        for slot in range(15):
            self.wait(self.own.at[slot], self.sent.at[2 + slot])


def scatter_shapes(down, ff=3200):
    block = (PAIR, HALF) if down else (ROWS, ff)
    vmem = [pltpu.VMEM((n, *block), BF16) for n in (CHIPS, CHIPS, 2, 2, 4, 4, 3)]
    return [*vmem, pltpu.SemaphoreType.DMA((16,)), pltpu.SemaphoreType.DMA((17,))]


def kept_shape(down, ff=3200):
    return jax.ShapeDtypeStruct((PAIR, HALF) if down else (ROWS, ff), BF16)


def term_shape(down, ff=3200):
    return jax.ShapeDtypeStruct((ff, 2 * HALF) if down else (CHIPS, 2, ROWS, ff), BF16)


def at_steps(hooks, steps):
    step = pl.program_id(0)
    if len(steps) == 2:
        step = step * steps[1] + pl.program_id(1)
    for when, hook in hooks:
        pl.when(step == when)(hook)


TILE = 640


def weight_job(hooks, a, g, out, down):
    steps = (out.shape[0] if down else out.shape[-1]) // TILE

    def body(a_ref, g_ref, out_ref):
        at_steps(hooks, (steps,))
        value = lax.dot_general(a_ref[...], g_ref[...], (((0,), (0,)), ((), ())), preferred_element_type=F32)
        out_ref[...] = value.astype(BF16).reshape(out_ref.shape)

    t = a.shape[0]
    if down:
        ins = [pl.BlockSpec((t, TILE), lambda j: (0, j)), pl.BlockSpec(g.shape, lambda j: (0, 0), pipeline_mode=pl.Buffered(1))]
        outs = [pl.BlockSpec((TILE, g.shape[1]), lambda j: (j, 0))]
    else:
        ins = [pl.BlockSpec(a.shape, lambda j: (0, 0), pipeline_mode=pl.Buffered(1)), pl.BlockSpec((t, TILE), lambda j: (0, j))]
        outs = [pl.BlockSpec((CHIPS, 2, ROWS, TILE), lambda j: (0, 0, 0, j))]
    pltpu.emit_pipeline(body, grid=(steps,), in_specs=ins, out_specs=outs)(a, g, out)


def input_job(hooks, m, dg, du, wg, wu, h, dh, out):
    t, d = out.shape
    steps = t // m

    def body(dg_ref, du_ref, wg_ref, wu_ref, h_ref, dh_ref, out_ref):
        at_steps(hooks, (steps,))
        da = [
            lax.dot_general(l[...], r[...], (((1,), (1,)), ((), ())), preferred_element_type=F32).astype(BF16)
            for l, r in ((dg_ref, wg_ref), (du_ref, wu_ref))
        ]
        out_ref[...] = dh_ref[...] + norm_back(h_ref[...], da[0] + da[1])

    hidden = pl.BlockSpec((m, dg.shape[1]), lambda i: (i, 0))
    weight = pl.BlockSpec(wg.shape, lambda i: (0, 0), pipeline_mode=pl.Buffered(1))
    row = pl.BlockSpec((m, d), lambda i: (i, 0))
    pltpu.emit_pipeline(
        body, grid=(steps,), in_specs=[hidden, hidden, weight, weight, row, row], out_specs=[row]
    )(dg, du, wg, wu, h, dh, out)


def later_kernel(h, dh, a, act, dg, du, wg, wu, down_out, gate_out, new, down, gate, up, *scratch):
    at = Place()
    greet(at)
    sd = Scatter(at, down, True, scratch[:7], *scratch[7:9], down_out)
    sg = Scatter(at, gate, False, scratch[9:16], *scratch[16:18], gate_out)
    weight_job([], act, dh, down, True)
    sd.start()
    weight_job([(2, sd.corners)], a, dg, gate, False)
    sg.start()
    weight_job([(1, sd.sides), (2, sg.corners)], a, du, up, False)
    hooks = [(0, sd.column), (1, sg.sides), (4, sd.finish), (5, sg.column)]
    input_job(hooks, 256, dg, du, wg, wu, h, dh, new)
    sg.finish()


def earlier_kernel(
    late, h, dh, a, act, g, u, wg, wu, wd, late_out, down_out, gate_out, up_out, new, dg, du, down, gate, up, *scratch
):
    at = Place()
    greet(at)
    sl = Scatter(at, late, False, scratch[:7], *scratch[7:9], late_out)
    sg = Scatter(at, gate, False, scratch[9:16], *scratch[16:18], gate_out)
    su = Scatter(at, up, False, scratch[18:25], *scratch[25:27], up_out)
    sd = Scatter(at, down, True, scratch[27:34], *scratch[34:36], down_out)
    sl.start()
    weight_job([(2, sl.corners)], act, dh, down, True)
    sd.start()

    def cotangents(_, dact, gate_ref, up_ref, dg_ref, du_ref):
        dg_ref[...], du_ref[...] = act_back(gate_ref[...], up_ref[...], dact.astype(BF16))

    hooks = [(0, sl.sides), (2, sd.corners), (4, sl.column), (6, sd.sides)]
    wide_job(hooks, dh, wd, True, cotangents, [g, u], [dg, du], 1024, 256)
    weight_job([(0, sd.column), (1, sl.finish)], a, dg, gate, False)
    sg.start()
    weight_job([(0, sd.finish), (1, sg.corners), (4, sg.sides)], a, du, up, False)
    su.start()
    hooks = [(1, su.corners), (2, sg.column), (4, su.sides), (7, su.column)]
    input_job(hooks, 256, dg, du, wg, wu, h, dh, new)
    sg.finish()
    su.finish()


def backward_call(kernel, index, ins, kept, spare, scratch):
    return pl.pallas_call(
        kernel,
        out_shape=[*kept, *spare],
        in_specs=[pl.BlockSpec(memory_space=pl.ANY)] * len(ins),
        out_specs=[pl.BlockSpec(memory_space=pltpu.VMEM)] * len(kept) + [pl.BlockSpec(memory_space=pl.ANY)] * len(spare),
        scratch_shapes=scratch,
        compiler_params=pltpu.CompilerParams(collective_id=index, has_side_effects=True, vmem_limit_bytes=VMEM_BYTES),
        name=f"backward{index}",
    )(*ins)


def scale_of(wide):
    return lax.rsqrt(jnp.mean(wide * wide, -1, keepdims=True) + 1e-6)


def norm(h):
    wide = h.astype(F32)
    return (wide * scale_of(wide)).astype(BF16)


def norm_back(h, da):
    wide, da = h.astype(F32), da.astype(F32)
    scale = scale_of(wide)
    inner = jnp.mean(wide * da, -1, keepdims=True)
    return (scale * da - wide * (scale * scale * scale * inner)).astype(BF16)


def sigmoid(gate):
    return 0.5 * jnp.tanh(0.5 * gate) + 0.5


def act_of(gate, up):
    return (gate * sigmoid(gate) * up).astype(BF16)


def act_back(gate, up, dact):
    dact = dact.astype(F32)
    sig = sigmoid(gate)
    soft = gate * sig
    return (dact * up * (sig + soft * (1 - sig))).astype(BF16), (dact * soft).astype(BF16)


def rows_job(hooks, steps, body, ins, outs):
    def cut(*refs):
        at_steps(hooks, (steps,))
        body(*refs)

    specs = [
        [pl.BlockSpec((t.shape[0] // steps, t.shape[1]), lambda i: (i, 0)) for t in part] for part in (ins, outs)
    ]
    pltpu.emit_pipeline(cut, grid=(steps,), in_specs=specs[0], out_specs=specs[1])(*ins, *outs)


def wide_job(hooks, a, w, transposed, body, ins, outs, m=1024, part=1024):
    t, d = a.shape
    ff = w.shape[0 if transposed else 1]
    grid = (ff // TILE, t // m)

    def cut(a_ref, w_ref, *refs):
        at_steps(hooks, grid)
        dims = (((1,), (1 if transposed else 0,)), ((), ()))
        for r in range(0, m, part):
            rows = pl.ds(pl.multiple_of(pl.program_id(1) * m + r, part), part)
            value = lax.dot_general(a_ref[rows], w_ref[...], dims, preferred_element_type=F32)
            body((pl.program_id(0), rows), value, *(ref.at[pl.ds(r, part)] for ref in refs))

    tile = pl.BlockSpec((m, TILE), lambda j, i: (i, j))
    weight = pl.BlockSpec((TILE, d), lambda j, i: (j, 0)) if transposed else pl.BlockSpec((d, TILE), lambda j, i: (0, j))
    pltpu.emit_pipeline(
        cut,
        grid=grid,
        in_specs=[pl.BlockSpec(a.shape, lambda j, i: (0, 0), pipeline_mode=pl.Buffered(1)), weight, *[tile] * len(ins)],
        out_specs=[tile] * len(outs),
    )(a, w, *ins, *outs)


def down_job(hooks, x, act, w, h, a):
    t, ff = act.shape
    m = 256
    steps = t // m

    def body(x_ref, act_ref, w_ref, h_ref, a_ref):
        at_steps(hooks, (steps,))
        value = jnp.dot(act_ref[...], w_ref[...], preferred_element_type=F32).astype(BF16)
        h_ref[...] = x_ref[...] + value
        a_ref[...] = norm(h_ref[...])

    row = pl.BlockSpec((m, x.shape[1]), lambda i: (i, 0))
    pltpu.emit_pipeline(
        body,
        grid=(steps,),
        in_specs=[
            row,
            pl.BlockSpec((m, ff), lambda i: (i, 0)),
            pl.BlockSpec(w.shape, lambda i: (0, 0), pipeline_mode=pl.Buffered(1)),
        ],
        out_specs=[row, row],
    )(x, act, w, h, a)


ORDER = (0, 1, 2, 5, 3, 4)


def norm_rows(x_ref, a_ref):
    a_ref[...] = norm(x_ref[...])


def forward_kernel(gate, up, down, x, dy, *refs):
    outs, (recv, other, sent, gate_at, dact_at) = refs[:15], refs[15:]
    wholes = outs[:6]
    a0, g0, u0, act0, h1, a1, dg1, du1, act1 = outs[6:]
    at = Place()
    greet(at)
    gathers = []
    for k in ORDER:
        src = (gate, up, down)[k % 3].at[k // 3]
        gathers.append(Gather(at, src, wholes[k], k % 3 == 2, recv.at[k], other.at[k], sent.at[k]))
    last = len(gathers) - 1

    def lines(k):
        return [gathers[k].lines] if k <= last else []

    def mine(k):
        return [gathers[k].mine] if k <= last else []

    def part(name, k, *steps):
        return [functools.partial(getattr(gathers[k], name), i) for i in steps] if 0 <= k <= last else []

    def during(k):
        n = k + 1
        return [
            part("plane", n, 0),
            part("column", n, 3),
            part("plane", n, 1),
            mine(n + 1) + lines(n + 2),
            part("plane", n, 2),
            part("plane", n, 3),
            part("column", n + 1, 1),
            part("corner", n, 0, 1),
            part("column", n + 1, 2),
            part("corner", n, 2, 3),
        ]

    def spread(k, steps, long):
        groups = during(k)
        hooks = [(min(steps - 1, j * steps * 27 // (10 * long)), hook) for j, group in enumerate(groups[:-1]) for hook in group]
        return hooks, groups[-1]

    gathers[0].lines()
    gathers[0].mine()
    gathers[1].lines()
    rows_job([], 4, norm_rows, [x], [a0])
    for hook in (
        part("column", 0, 1)
        + part("plane", 0, 0)
        + part("column", 0, 2)
        + part("plane", 0, 1)
        + part("column", 0, 3)
        + part("plane", 0, 2)
        + mine(1)
        + lines(2)
        + part("plane", 0, 3)
        + part("column", 1, 1)
        + part("corner", 0, 0, 1)
        + part("column", 1, 2)
        + part("corner", 0, 2, 3)
    ):
        hook()

    def gate_0(here, value, out_ref):
        gate_at[here] = value
        out_ref[...] = value

    def up_0(here, value, up_ref, act_ref):
        up_ref[...] = value
        act_ref[...] = act_of(gate_at[here], value)

    def dact_1(here, value):
        dact_at[here] = value.astype(BF16)

    def gate_1(here, value):
        gate_at[here] = value

    def up_1(here, value, dg_ref, du_ref, act_ref):
        gate = gate_at[here]
        act_ref[...] = act_of(gate, value)
        dg_ref[...], du_ref[...] = act_back(gate, value, dact_at[here])

    w = [g.whole for g in gathers]
    jobs = [
        lambda hooks: wide_job(hooks, a0, w[0], False, gate_0, [], [g0], 1024, 256),
        lambda hooks: wide_job(hooks, a0, w[1], False, up_0, [], [u0, act0], 1024, 256),
        lambda hooks: down_job(hooks, x, act0, w[2], h1, a1),
        lambda hooks: wide_job(hooks, dy, w[3], True, dact_1, [], [], 1024, 256),
        lambda hooks: wide_job(hooks, a1, w[4], False, gate_1, [], [], 1024, 256),
        lambda hooks: wide_job(hooks, a1, w[5], False, up_1, [], [dg1, du1, act1], 1024, 256),
    ]
    steps = ((10, 25), (10, 26), (8, 23), (10, 23), (10, 23), (10, 25))
    for k, job in enumerate(jobs):
        gathers[k].arrived()
        hooks, rest = spread(k, *steps[k])
        job(hooks)
        for hook in rest:
            hook()
    for g in gathers:
        g.settled()


def forward(gate, up, down, x, dy):
    t, d = x.shape
    ff = gate.shape[-1]
    weights = [jax.ShapeDtypeStruct(s, BF16) for s in ((d, ff), (d, ff), (ff, d))] * 2
    row, wide, exact = (jax.ShapeDtypeStruct(s, t_) for s, t_ in (((t, d), BF16), ((t, ff), BF16), ((t, ff), F32)))
    outs = [*weights, row, exact, exact, wide, row, row, wide, wide, wide]
    return pl.pallas_call(
        forward_kernel,
        out_shape=outs,
        in_specs=[pl.BlockSpec(memory_space=pltpu.VMEM)] * 3 + [pl.BlockSpec(memory_space=pl.ANY)] * 2,
        out_specs=[pl.BlockSpec(memory_space=pl.ANY)] * len(outs),
        scratch_shapes=[
            pltpu.SemaphoreType.DMA((6, CHIPS)),
            pltpu.SemaphoreType.DMA((6,)),
            pltpu.SemaphoreType.DMA((6, 3)),
            pltpu.VMEM((ff // TILE, t, TILE), F32),
            pltpu.VMEM((ff // TILE, t, TILE), BF16),
        ],
        compiler_params=pltpu.CompilerParams(collective_id=0, has_side_effects=True, vmem_limit_bytes=VMEM_BYTES),
        name="forward",
    )(gate, up, down, x, dy)


def step_of_a_device(x, dy, gate, up, down):
    x, dy = x[0], dy[0]
    c = lax.axis_index("dp") % 2
    pairs = [[2 * i, 2 * i + 1] for i in range(CHIPS)]
    both = lax.all_gather(down, "dp", axis_index_groups=pairs, axis=1, tiled=True)
    mine = lax.dynamic_slice_in_dim(both, c * HALF, HALF, axis=2)
    wg0, wu0, wd0, wg1, wu1, wd1, a0, g0, u0, act0, h1, a1, dg1, du1, act1 = forward(gate, up, mine, x, dy)
    state = jax.ShapeDtypeStruct(x.shape, BF16)
    hidden = jax.ShapeDtypeStruct(dg1.shape, BF16)
    row, col = term_shape(False), term_shape(True)
    down1, gate1, dh1, _, _, up_term = backward_call(
        later_kernel,
        1,
        (h1, dy, a1, act1, dg1, du1, wg1, wu1),
        (kept_shape(True), kept_shape(False)),
        (state, col, row, row),
        scatter_shapes(True) + scatter_shapes(False),
    )
    up1, down0, gate0, up0, dx, *_ = backward_call(
        earlier_kernel,
        2,
        (up_term, x, dh1, a0, act0, g0, u0, wg0, wu0, wd0),
        (kept_shape(False), kept_shape(True), kept_shape(False), kept_shape(False)),
        (state, hidden, hidden, col, row, row),
        scatter_shapes(False) * 3 + scatter_shapes(True),
    )
    r0, r1 = (gate0, up0, down0), (gate1, up1, down1)
    dgate, dup, ddown = (jnp.stack([p, q]) for p, q in zip(r0, r1))
    ddown = lax.all_gather(ddown, "dp", axis_index_groups=pairs, axis=2, tiled=True)
    ddown = lax.dynamic_slice_in_dim(ddown, c * (PAIR // 2), PAIR // 2, axis=1)
    return dx[None], dgate, dup, ddown


def solution(mesh):
    seq, rows = P(("rep", "dp"), None, None), P(None, "dp", None)
    grads = P("rep", "dp", None)
    return jax.shard_map(
        step_of_a_device,
        mesh=mesh,
        in_specs=(seq, seq, rows, rows, rows),
        out_specs=(seq, grads, grads, grads),
        check_vma=False,
    )
```
